512 devices in a mesh: verts: 128 (over z, y, core), modes: 4 (over x).
Axes of the slice: x: 4, y: 4, z: 16, core: 2. Of those that a mesh axis runs over, the one named last changes fastest.
Arguments:
- reduced_coords: float32 [256], P('modes'), may hold values from -4 to 4
- mode_basis: bfloat16 [256, 3, 131072], P('modes', None, 'verts'), may hold values from -0.375 to 0.375
- rest_shape: float32 [3, 131072], P(None, 'verts'), may hold values from -6 to 6
- stiffness: float32 [131072], P('verts'), may hold values from 0.2 to 2
- send_slots: int32 [128, 128, 16], P('verts'), may hold values from 0 to 1023
- pair_peer: int32 [128, 2, 1024], P('verts'), may hold values from 0 to 127
- pair_slot: int32 [128, 2, 1024], P('verts'), may hold values from 0 to 15
- pair_count: int32 [128], P('verts'), may hold values from 1 to 1024, 65536 in all
Outputs:
- hessian: float32 [256, 256], P('modes')
- gradient: float32 [256], P('modes')
The draws below stay inside these ranges and needn't reach their ends.
Inputs may be any that keep to these rules, and one draw needn't show every extreme that they name: `send_slots`: indices may repeat. `pair_count`: the counts sum to 128 * 512 and the busiest owner has all 1024 slots live; slots at and beyond an owner's count hold valid but unused indices.
All inputs are finite; a program needn't handle non-finite values. No bound on the sum of `pair_count` on one device may be relied on, other than what follows from the above.
Results may differ from the reference program's by a relative error of at most 0.0046.
Values may be sent and summed in bfloat16 or wider, within the bound.
A program may use at most 64 MiB of HBM per device.

```python
import math
import jax
import jax.numpy as jnp
import numpy as np
from jax import lax

M = 256
VB = 1024
C = 16
P_SIZE = 1024
V = 131072
N_VERTS = 128


def plant(result, stream_key, least, high):
    longest = result.shape.index(max(result.shape))
    spots = []
    for shift in (0, 1):
        where = [jax.random.randint(jax.random.fold_in(stream_key, axis), (), 0, length) for axis, length in enumerate(result.shape)]
        where[longest] = (where[longest] + shift) % result.shape[longest]
        spots.append(tuple(where))
    return result.at[spots[0]].set(least).at[spots[1]].set(high)


def levels(key, dims, split, smallest, high):
    def one(position, shards_of):
        heights = jax.random.uniform(jax.random.fold_in(jax.random.fold_in(key, 6), position), (shards_of,), jnp.float32, smallest / len(split), high / len(split))
        return jnp.repeat(jnp.exp(heights), dims[position] // shards_of).reshape((-1,) + (1,) * (len(dims) - position - 1))

    gain = one(*split[0])
    for cut in split[1:]:
        gain = gain * one(*cut)
    return gain


def profile(count, total, bound, slope):
    weights = [(1 << 20) // math.isqrt(rank ** slope) + 1 for rank in range(2, count + 1)]
    surplus, holding = total - bound - (count - 1), [1] * (count - 1)
    while surplus > 0:
        free = [i for i in range(count - 1) if holding[i] < bound]
        mass, left = sum([weights[i] for i in free]), surplus
        for i in free:
            addition = min(bound - holding[i], max(1, left * weights[i] // mass), surplus)
            holding[i] = holding[i] + addition
            surplus = surplus - addition
    return np.array([bound] + holding)


def uneven_parts(key, count, total, bound, slope):
    if count == 2:
        one = jax.random.randint(key, (), max(1, total - bound), min(bound, total - 1) + 1)
        return jnp.stack([one, total - one])
    tallies = jnp.asarray(profile(count, total, bound, slope), jnp.int32)
    twos = (count - 1) // 2
    source_of, taker = tallies[1:1 + 2 * twos:2], tallies[2:2 + 2 * twos:2]
    room = jnp.minimum(source_of - 1, bound - taker)
    moved = jax.random.randint(jax.random.fold_in(key, 1), (twos,), 0, 1 << 20) % (room + 1)
    tallies = tallies.at[1:1 + 2 * twos:2].set(source_of - moved).at[2:2 + 2 * twos:2].set(taker + moved)
    return tallies[jax.random.permutation(jax.random.fold_in(key, 2), count)]


def normal_values(own_key, dims, deviation, reach, cuts=(), held_as=jnp.bfloat16):
    result = deviation * jax.random.normal(own_key, dims, jnp.float32)
    if cuts:
        result = result * levels(own_key, dims, cuts, -0.22, 0.18)
    return jnp.clip(result, -reach, reach).astype(held_as)


def setup_inputs(seed: int = 0) -> dict:
    streams_of = jax.random.split(jax.random.key(seed), 9)
    reduced_coords = normal_values(streams_of[0], (M,), 0.3, 4.0, ((0, 4),), jnp.float32)
    mode_basis = normal_values(streams_of[1], (M, 3, V), M ** -0.5, 0.375, ((0, 4), (2, 128)))
    rest_shape = normal_values(streams_of[2], (3, V), 0.5, 6.0, ((1, 128),), jnp.float32)
    stiffness = jnp.clip(jnp.exp(math.log(2.0) - 2.3025851 * jax.random.uniform(streams_of[3], (V,), jnp.float32) ** levels(streams_of[3], (V,), ((0, 128),), -0.2, 0.2)), 0.2, 2.0)
    send_slots = plant(jax.random.randint(streams_of[4], (N_VERTS, N_VERTS, C), 0, VB), jax.random.fold_in(streams_of[4], 1), 0, VB - 1).astype(jnp.int32)
    pair_peer = plant(jax.random.randint(streams_of[5], (N_VERTS, 2, P_SIZE), 0, N_VERTS), jax.random.fold_in(streams_of[5], 1), 0, N_VERTS - 1).astype(jnp.int32)
    pair_slot = plant(jax.random.randint(streams_of[6], (N_VERTS, 2, P_SIZE), 0, C), jax.random.fold_in(streams_of[6], 1), 0, C - 1).astype(jnp.int32)
    pair_count = uneven_parts(streams_of[7], N_VERTS, N_VERTS * P_SIZE // 2, P_SIZE, 2).astype(jnp.int32)
    return {"reduced_coords": reduced_coords, "mode_basis": mode_basis, "rest_shape": rest_shape, "stiffness": stiffness, "send_slots": send_slots, "pair_peer": pair_peer, "pair_slot": pair_slot, "pair_count": pair_count}


highest = lax.Precision.HIGHEST
barrier_reach = 1.5
gap_offset = 0.1

def barrier_slopes(distance):
    excess = distance - barrier_reach
    ratio_log = jnp.log(distance / barrier_reach)
    slope_term = -(2.0 * excess * ratio_log + excess * excess / distance)
    curvature = -(2.0 * ratio_log + 4.0 * excess / distance - excess * excess / (distance * distance))
    inside = distance < barrier_reach
    return (jnp.where(inside, slope_term, 0.0), jnp.where(inside, curvature, 0.0))

def outer_sum(left_rows, right_rows):
    return lax.dot_general(left_rows.astype(jnp.float32), right_rows.astype(jnp.float32), (((1,), (1,)), ((), ())), precision=highest, preferred_element_type=jnp.float32)

def spring_terms(displacement, stiffness):
    radius = jnp.sqrt(1.0 + lax.optimization_barrier(jnp.sum(displacement * displacement, axis=0)))
    spring_rate = stiffness / radius
    return (spring_rate, -spring_rate / (radius * radius), spring_rate * displacement)

def elastic_left(basis_block, displacement, spring_rate, curvature_rate):
    mode_count, _, vertex_count = basis_block.shape
    projected = lax.optimization_barrier(jnp.sum(basis_block.astype(jnp.float32) * displacement[None], axis=1))
    scaled = (spring_rate * basis_block.astype(jnp.float32)).astype(jnp.bfloat16)
    return jnp.concatenate([scaled.reshape(mode_count, 3 * vertex_count), (curvature_rate * projected).astype(jnp.bfloat16)], axis=1)

def elastic_right(basis_block, displacement):
    mode_count, _, vertex_count = basis_block.shape
    projected = lax.optimization_barrier(jnp.sum(basis_block.astype(jnp.float32) * displacement[None], axis=1))
    return jnp.concatenate([basis_block.reshape(mode_count, 3 * vertex_count), projected.astype(jnp.bfloat16)], axis=1)

def contact_terms(rows_first, rows_second, separation, active):
    mode_count, _, slot_total = rows_first.shape
    distance = lax.optimization_barrier(jnp.sum(separation * separation, axis=0)) + gap_offset
    slope_term, curvature = barrier_slopes(distance)
    slope_term = slope_term * active
    curvature = curvature * active
    difference = rows_first.astype(jnp.float32) - rows_second.astype(jnp.float32)
    leverage = lax.optimization_barrier(jnp.sum(difference * separation[None], axis=1))
    left_rows = jnp.concatenate([(2.0 * slope_term * difference).astype(jnp.bfloat16).reshape(mode_count, 3 * slot_total), (4.0 * curvature * leverage).astype(jnp.bfloat16)], axis=1)
    right_rows = jnp.concatenate([difference.astype(jnp.bfloat16).reshape(mode_count, 3 * slot_total), leverage.astype(jnp.bfloat16)], axis=1)
    contact_grad = lax.optimization_barrier(jnp.sum(difference * (2.0 * slope_term * separation)[None], axis=(1, 2)))
    return (left_rows, right_rows, contact_grad)

def reference(reduced_coords, mode_basis, rest_shape, stiffness, send_slots, pair_peer, pair_slot, pair_count):
    mode_count = mode_basis.shape[0]
    total = rest_shape.shape[1]
    blocks = N_VERTS
    vertex_count = total // blocks
    slot_total = pair_peer.shape[2]

    def rebuild(block_index):
        first_row = block_index * vertex_count
        basis_block = lax.dynamic_slice_in_dim(mode_basis, first_row, vertex_count, 2)
        rest_block = lax.dynamic_slice_in_dim(rest_shape, first_row, vertex_count, 1)
        moved = jnp.dot(reduced_coords, basis_block.reshape(mode_count, 3 * vertex_count).astype(jnp.float32), precision=highest, preferred_element_type=jnp.float32)
        return rest_block + moved.reshape(3, vertex_count)
    stacked = lax.map(rebuild, jnp.arange(blocks, dtype=jnp.int32))
    positions = jnp.transpose(stacked, (1, 0, 2)).reshape(3, total)

    def elastic_step(totals, block_index):
        first_row = block_index * vertex_count
        basis_block = lax.dynamic_slice_in_dim(mode_basis, first_row, vertex_count, 2)
        rest_block = lax.dynamic_slice_in_dim(rest_shape, first_row, vertex_count, 1)
        stiff_block = lax.dynamic_slice_in_dim(stiffness, first_row, vertex_count, 0)
        displacement = stacked[block_index] - rest_block
        spring_rate, curvature_rate, elastic_force = spring_terms(displacement, stiff_block)
        left_rows = elastic_left(basis_block, displacement, spring_rate, curvature_rate)
        right_rows = elastic_right(basis_block, displacement)
        grad_term = jnp.dot(basis_block.reshape(mode_count, 3 * vertex_count).astype(jnp.float32), elastic_force.reshape(3 * vertex_count), precision=highest, preferred_element_type=jnp.float32)
        return ((totals[0] + outer_sum(left_rows, right_rows), totals[1] + grad_term), None)
    initial = (jnp.zeros((mode_count, mode_count), jnp.float32), jnp.zeros((mode_count,), jnp.float32))
    totals, _ = lax.scan(elastic_step, initial, jnp.arange(blocks, dtype=jnp.int32))

    def contact_step(totals, owner_index):
        senders = pair_peer[owner_index]
        chosen = send_slots[senders, owner_index, pair_slot[owner_index]]
        vertex_ids = (senders * vertex_count + chosen).reshape(-1).astype(jnp.int32)
        pos_ends = jnp.take(positions, vertex_ids, axis=1).reshape(3, 2, slot_total)
        row_ends = jnp.take(mode_basis, vertex_ids, axis=2).reshape(mode_count, 3, 2, slot_total)
        separation = pos_ends[:, 0] - pos_ends[:, 1]
        active = (jnp.arange(slot_total, dtype=jnp.int32) < pair_count[owner_index]).astype(jnp.float32)
        left_rows, right_rows, contact_grad = contact_terms(row_ends[:, :, 0], row_ends[:, :, 1], separation, active)
        return ((totals[0] + outer_sum(left_rows, right_rows), totals[1] + contact_grad), None)
    totals, _ = lax.scan(contact_step, totals, jnp.arange(blocks, dtype=jnp.int32))
    factor = mode_count / (3.0 * total)
    return (totals[0] * factor, totals[1] * factor)
```

```python
import jax
import jax.numpy as jnp
from jax import lax
from jax.experimental import pallas as pl
from jax.experimental.pallas import tpu as pltpu
from jax.sharding import Mesh
from jax.sharding import PartitionSpec as P

VERTS = ("z", "y", "c")
MESH = pl.DeviceIdType.MESH
NZ, NS, NX = 16, 8, 4
NP = NX * NS
LM, LC = 64, 192
NV, NPAIR, NSLOT = 1024, 1024, 16
Q = 256
ROWS = 24
GROUP = 4
f32, bf16 = jnp.float32, jnp.bfloat16

barrier_reach = 1.5
gap_offset = 0.1


def split3(v):
    hi = v.astype(bf16).astype(f32)
    mid = (v - hi).astype(bf16).astype(f32)
    return hi, mid, v - hi - mid


def dot_nt(a, b):
    return lax.dot_general(a, b, (((1,), (1,)), ((), ())), preferred_element_type=f32)


def dot_nn(a, b):
    return lax.dot_general(a, b, (((1,), (0,)), ((), ())), preferred_element_type=f32)


def offset_of(n):
    half = n // 2
    return 8 + half - (n % 2) * (2 * half + 1)


def barrier_slopes(distance):
    excess = distance - barrier_reach
    ratio_log = jnp.log(distance / barrier_reach)
    slope_term = -(2.0 * excess * ratio_log + excess * excess / distance)
    curvature = -(2.0 * ratio_log + 4.0 * excess / distance - excess * excess / (distance * distance))
    inside = distance < barrier_reach
    return jnp.where(inside, slope_term, 0.0), jnp.where(inside, curvature, 0.0)


def accumulate(rows_ref, s, scale, bend, hess, grad, first):
    rows = rows_ref[...]
    lever = jnp.zeros((NX * LM, Q), f32)
    total = None
    slopes = None
    for k in range(3):
        xb = rows[:, LM * k : LM * (k + 1), :].reshape(NX * LM, Q)
        x = xb.astype(f32)
        sk = s[k : k + 1, :]
        lever = lever + x * sk
        part = dot_nt((x * scale).astype(bf16), xb)
        total = part if total is None else total + part
        hi, mid, lo = split3(scale * sk)
        force = jnp.concatenate([hi, mid, lo, jnp.zeros((13, Q), f32)], axis=0).astype(bf16)
        gpart = dot_nt(force, xb)
        slopes = gpart if slopes is None else slopes + gpart
    total = total + dot_nt((lever * bend).astype(bf16), lever.astype(bf16))
    slopes = jnp.sum(slopes, axis=0, keepdims=True)
    if first:
        hess[...] = total
        grad[...] = slopes
    else:
        hess[...] = hess[...] + total
        grad[...] = grad[...] + slopes


def kernel(
    factor,
    basis_ref, coeff_ref, rest_ref, stiff_ref, slots_ref, ends_ref, count_ref,
    out_h, out_g,
    wide, obuf, stage, rows_in, restg, restp, resta, restz,
    part_s, xb, xp, acc, dsend, usend, xd, xu,
    hess, grad, hsend, hplane, zsend, hz, csend, hc,
    p1_s, p1_r, ri_s, ri_r, rz_s, rz_r, zm_s, zm_r,
    x_s, x_r, a_s, a_r, b_s, b_r, c_s, c_r,
):
    z, y, c, x = (lax.axis_index(n) for n in ("z", "y", "c", "x"))
    s = y * 2 + c
    p = x * NS + s

    def place(xq, sq):
        return {"x": xq, "y": sq // 2, "c": lax.rem(sq, 2)}

    def plane_peer(k):
        q = lax.rem(p + k, NP)
        return q, place(q // NS, lax.rem(q, NS))

    def near_peer(k):
        q = lax.rem(s + k, NS)
        return q, {"y": q // 2, "c": lax.rem(q, 2)}

    def remote(src, dst, ssem, rsem, where):
        return pltpu.make_async_remote_copy(src, dst, ssem, rsem, device_id=where, device_id_type=MESH)

    bar = pltpu.get_barrier_semaphore()

    @pl.loop(1, NZ)
    def _(k):
        pl.semaphore_signal(bar, inc=1, device_id={"z": lax.rem(z + k, NZ)}, device_id_type=MESH)

    @pl.loop(1, NP)
    def _(k):
        pl.semaphore_signal(bar, inc=1, device_id=plane_peer(k)[1], device_id_type=MESH)

    wide[0:LC, :] = basis_ref[...]
    wide[LC:Q, :] = jnp.zeros((Q - LC, NV), bf16)
    rest = rest_ref[...]
    mine = jnp.where(x == 0, rest[0:1], jnp.where(x == 1, rest[1:2], jnp.where(x == 2, rest[2:3], 0.0)))
    hi, mid, lo = split3(mine)
    rest_rows = jnp.concatenate([hi, mid, lo, jnp.zeros((13, NV), f32)], axis=0).astype(bf16)
    lane = lax.broadcasted_iota(jnp.int32, (128, 128), 1).astype(f32)

    @pl.loop(0, NZ // GROUP)
    def _(g):
        hots = []
        for i in range(GROUP):
            zq = lax.rem(z + offset_of(g * GROUP + i), NZ)
            row = slots_ref[pl.ds(zq, 1), :].astype(f32)
            col = jnp.transpose(jnp.broadcast_to(row, (128, 128)))
            blocks = [jnp.where(col == lane + 128.0 * b, 1.0, 0.0).astype(bf16) for b in range(NV // 128)]
            hots.append(jnp.concatenate(blocks, axis=1))
        hot = jnp.concatenate(hots, axis=0)
        picked = dot_nt(hot, wide[...])
        tail = picked[:, 128:256]
        turned = pltpu.roll(tail, 64, 1)
        tail = tail.reshape(GROUP * NS, 2, 8, 128)[:, 0] + turned.reshape(GROUP * NS, 2, 8, 128)[:, 1]
        chunk = jnp.concatenate([picked[:, 0:128].reshape(GROUP * NS, 16, 128), tail], axis=1)
        chunk = chunk.astype(bf16).reshape(GROUP, NS, ROWS, 128)
        rests = jnp.sum(dot_nt(rest_rows, hot), axis=0, keepdims=True)
        for i in range(GROUP):
            n = g * GROUP + i
            obuf[:, pl.ds(n, 1)] = chunk[i][:, None]
            restg[pl.ds(n, 1), :] = rests[:, 128 * i : 128 * (i + 1)]

    coeff = coeff_ref[...]
    moved = dot_nn(coeff, basis_ref[...])
    part_s[...] = moved[0:8] + moved[8:16] + moved[16:24]

    pl.semaphore_wait(bar, NZ - 1 + NP - 1)

    for g in range(NZ // GROUP):
        span = pl.ds(g * GROUP, GROUP)

        @pl.loop(1, NS)
        def _(k):
            q, where = near_peer(k)
            remote(obuf.at[q, span], stage.at[span, s], p1_s.at[g], p1_r.at[g], where).start()

    @pl.loop(1, NS)
    def _(k):
        _q, where = near_peer(k)
        remote(restg, restp.at[s], ri_s, ri_r, where).start()

    @pl.loop(1, NX)
    def _(k):
        q = lax.rem(x + k, NX)
        cols = pl.ds(pl.multiple_of(q * Q, Q), Q)
        remote(basis_ref.at[:, cols], xb.at[x], x_s.at[0], x_r.at[0], {"x": q}).start()
        remote(part_s.at[:, cols], xp.at[x], x_s.at[1], x_r.at[1], {"x": q}).start()

    own = pl.ds(pl.multiple_of(x * Q, Q), Q)
    xb[x] = basis_ref[:, own]
    xp[x] = part_s[:, own]
    stage[:, pl.ds(s, 1)] = obuf[s][:, None]
    restp[s] = restg[...]

    for g in range(NZ // GROUP):
        whole = obuf.at[pl.ds(0, NS - 1), pl.ds(0, GROUP)]
        remote(whole, whole, p1_s.at[g], p1_r.at[g], {"z": z}).wait_recv()
        for i in range(GROUP):
            n = g * GROUP + i
            if n < NZ - 1:
                remote(stage.at[n], rows_in.at[n], zm_s, zm_r.at[n], {"z": lax.rem(z + offset_of(n), NZ)}).start()
        if g == 0:
            remote(restp.at[pl.ds(0, NS - 1)], restp.at[pl.ds(0, NS - 1)], ri_s, ri_r, {"z": z}).wait_recv()
            place_of = lax.broadcasted_iota(jnp.int32, (NZ, 128), 1) // NSLOT
            gathered = jnp.zeros((NZ, 128), f32)
            for q in range(NS):
                shift = lax.rem((q - s + NS) * NSLOT, 128)
                gathered = jnp.where(place_of == q, pltpu.roll(restp[q], shift, 1), gathered)
            resta[...] = gathered.reshape(NZ, 1, 128)
            for n in range(NZ - 1):
                remote(resta.at[n], restz.at[n], rz_s, rz_r, {"z": lax.rem(z + offset_of(n), NZ)}).start()
            restz[NZ - 1] = resta[NZ - 1]
    rows_in[NZ - 1] = stage[NZ - 1]

    for i, buf in ((0, xb), (1, xp)):
        remote(buf.at[pl.ds(0, NX - 1)], buf.at[pl.ds(0, NX - 1)], x_s.at[i], x_r.at[i], {"z": z}).wait_recv()
    disp = xp[0] + xp[1] + xp[2] + xp[3]
    square = 1.0 + disp[0:1] * disp[0:1] + disp[1:2] * disp[1:2] + disp[2:3] * disp[2:3]
    rate = stiff_ref[:, own] / jnp.sqrt(square)
    accumulate(xb, disp, rate, -rate / square, hess, grad, True)

    acc[...] = jnp.zeros_like(acc)
    remote(resta.at[pl.ds(0, NZ - 1)], restz.at[pl.ds(0, NZ - 1)], rz_s, rz_r, {"z": z}).wait_recv()
    pick = lax.broadcasted_iota(jnp.int32, (8, 128), 0) == x
    code = lax.broadcasted_iota(jnp.int32, (128, NPAIR), 0)

    def absorb(n):
        base = lax.rem(z + NZ - offset_of(n), NZ) * 128
        first = jnp.where(ends_ref[0:1, :] - base == code, 1.0, 0.0)
        second = jnp.where(ends_ref[1:2, :] - base == code, 1.0, 0.0)
        return (first - second).astype(bf16)

    def consume(n, choose):
        got = rows_in[n].astype(f32)
        head = got[:, 0:16].reshape(128, 128)
        tail = got[:, 16:24]
        turned = pltpu.roll(tail.reshape(64, 128), 64, 1).reshape(NS, 1, 8, 128)
        tail = jnp.concatenate([tail.reshape(NS, 1, 8, 128), turned], axis=1).reshape(128, 128)
        cols = jnp.concatenate([jnp.transpose(head), jnp.transpose(tail)[0:LM]], axis=0).astype(bf16)
        pos = dot_nn(coeff, cols)
        pos = pos[0:8] + pos[8:16] + pos[16:24] + jnp.where(pick, restz[n], 0.0)
        hi, mid, lo = split3(pos)
        pos = jnp.concatenate([hi, mid, lo, jnp.zeros((8, 128), f32)], axis=0).astype(bf16)
        acc[...] = acc[...] + dot_nn(jnp.concatenate([cols, pos], axis=0), choose)

    consume(NZ - 1, absorb(NZ - 1))

    @pl.loop(0, NZ - 1)
    def _(n):
        choose = absorb(n)
        remote(stage.at[n], rows_in.at[n], zm_s, zm_r.at[n], {"z": z}).wait_recv()
        consume(n, choose)

    dsend[...] = acc[0:LC, :].astype(bf16)
    usend[...] = acc[LC : LC + 8, :] + acc[LC + 8 : LC + 16, :] + acc[LC + 16 : LC + 24, :]

    @pl.loop(1, NX)
    def _(k):
        q = lax.rem(x + k, NX)
        cols = pl.ds(pl.multiple_of(q * Q, Q), Q)
        remote(usend.at[:, cols], xu.at[x], x_s.at[3], x_r.at[3], {"x": q}).start()
        remote(dsend.at[:, cols], xd.at[x], x_s.at[2], x_r.at[2], {"x": q}).start()

    xd[x] = dsend[:, own]
    xu[x] = usend[:, own]
    remote(xu.at[pl.ds(0, NX - 1)], xu.at[pl.ds(0, NX - 1)], x_s.at[3], x_r.at[3], {"z": z}).wait_recv()
    gap = xu[0] + xu[1] + xu[2] + xu[3]
    distance = gap[0:1] * gap[0:1] + gap[1:2] * gap[1:2] + gap[2:3] * gap[2:3] + gap_offset
    slope, bend = barrier_slopes(distance)
    live = lax.broadcasted_iota(jnp.int32, (1, Q), 1) + x * Q < count_ref[0]
    slope = jnp.where(live, slope, 0.0)
    bend = jnp.where(live, bend, 0.0)
    remote(xd.at[pl.ds(0, NX - 1)], xd.at[pl.ds(0, NX - 1)], x_s.at[2], x_r.at[2], {"z": z}).wait_recv()
    accumulate(xd, gap, 2.0 * slope, 4.0 * bend, hess, grad, False)

    def packed_grad(row):
        hi = row.astype(bf16).astype(f32)
        lo = row - hi
        return jnp.concatenate(
            [hi[:, 0:128], hi[:, 128:256], lo[:, 0:128], lo[:, 128:256], jnp.zeros((4, 128), f32)], axis=0
        )

    h = hess[...]
    tail = jnp.broadcast_to(packed_grad(grad[...])[None], (NP, 8, 128))
    hsend[...] = jnp.concatenate(
        [h[:, 0:128].reshape(NP, 8, 128), h[:, 128:256].reshape(NP, 8, 128), tail], axis=1
    ).astype(bf16)

    @pl.loop(1, NP)
    def _(k):
        q, where = plane_peer(k)
        remote(hsend.at[q], hplane.at[p], a_s, a_r, where).start()

    hplane[p] = hsend[p]
    remote(hsend.at[pl.ds(0, NP - 1)], hplane.at[pl.ds(0, NP - 1)], a_s, a_r, {"z": z}).wait_recv()
    total = jnp.sum(hplane[...].astype(f32), axis=0)
    g0, g1 = total[16:17] + total[18:19], total[17:18] + total[19:20]
    zsend[...] = jnp.concatenate([total[0:16], packed_grad(jnp.concatenate([g0, g1], axis=1))], axis=0).astype(bf16)

    @pl.loop(1, NZ)
    def _(k):
        remote(zsend, hz.at[z], b_s, b_r, {"z": lax.rem(z + k, NZ)}).start()

    hz[z] = zsend[...]
    remote(hz.at[pl.ds(0, NZ - 1)], hz.at[pl.ds(0, NZ - 1)], b_s, b_r, {"z": z}).wait_recv()
    total = jnp.sum(hz[...].astype(f32), axis=0) * factor
    csend[...] = total[0:16]

    @pl.loop(1, NS)
    def _(k):
        _q, where = near_peer(k)
        remote(csend, hc.at[s], c_s, c_r, where).start()

    hc[s] = csend[...]
    g0, g1 = total[16:17] + total[18:19], total[17:18] + total[19:20]
    half = jnp.where(x >= 2, g1, g0)
    half = jnp.where(lax.rem(x, 2) == 1, pltpu.roll(jnp.broadcast_to(half, (8, 128)), 64, 1), half)
    out_g[...] = half
    remote(hc.at[pl.ds(0, NS - 1)], hc.at[pl.ds(0, NS - 1)], c_s, c_r, {"z": z}).wait_recv()
    out_h[:, 0:128] = hc[:, 0:8, :].reshape(LM, 128)
    out_h[:, 128:256] = hc[:, 8:16, :].reshape(LM, 128)

    for g in range(NZ // GROUP):
        whole = obuf.at[pl.ds(0, NS - 1), pl.ds(0, GROUP)]
        remote(whole, whole, p1_s.at[g], p1_r.at[g], {"z": z}).wait_send()
    for src, sem in (
        (restp.at[pl.ds(0, NS - 1)], ri_s),
        (resta.at[pl.ds(0, NZ - 1)], rz_s),
        (stage.at[pl.ds(0, NZ - 1)], zm_s),
        (xb.at[pl.ds(0, NX - 1)], x_s.at[0]),
        (xp.at[pl.ds(0, NX - 1)], x_s.at[1]),
        (xd.at[pl.ds(0, NX - 1)], x_s.at[2]),
        (xu.at[pl.ds(0, NX - 1)], x_s.at[3]),
        (hsend.at[pl.ds(0, NP - 1)], a_s),
        (hz.at[pl.ds(0, NZ - 1)], b_s),
        (hc.at[pl.ds(0, NS - 1)], c_s),
    ):
        remote(src, src, sem, c_r, {"z": z}).wait_send()


def step(factor, *operands):
    dma = pltpu.SemaphoreType.DMA
    scratch = [
        pltpu.VMEM((Q, NV), bf16),
        pltpu.VMEM((NS, NZ, ROWS, 128), bf16),
        pltpu.VMEM((NZ, NS, ROWS, 128), bf16),
        pltpu.VMEM((NZ, NS, ROWS, 128), bf16),
        pltpu.VMEM((NZ, 128), f32),
        pltpu.VMEM((NS, NZ, 128), f32),
        pltpu.VMEM((NZ, 1, 128), f32),
        pltpu.VMEM((NZ, 1, 128), f32),
        pltpu.VMEM((8, NV), f32),
        pltpu.VMEM((NX, LC, Q), bf16),
        pltpu.VMEM((NX, 8, Q), f32),
        pltpu.VMEM((LC + 32, NPAIR), f32),
        pltpu.VMEM((LC, NPAIR), bf16),
        pltpu.VMEM((8, NPAIR), f32),
        pltpu.VMEM((NX, LC, Q), bf16),
        pltpu.VMEM((NX, 8, Q), f32),
        pltpu.VMEM((NX * LM, NX * LM), f32),
        pltpu.VMEM((1, NX * LM), f32),
        pltpu.VMEM((NP, ROWS, 128), bf16),
        pltpu.VMEM((NP, ROWS, 128), bf16),
        pltpu.VMEM((ROWS, 128), bf16),
        pltpu.VMEM((NZ, ROWS, 128), bf16),
        pltpu.VMEM((16, 128), f32),
        pltpu.VMEM((NS, 16, 128), f32),
        dma((NZ // GROUP,)), dma((NZ // GROUP,)), dma, dma, dma, dma, dma, dma((NZ,)),
        dma((4,)), dma((4,)), dma, dma, dma, dma, dma, dma,
    ]
    vmem = pl.BlockSpec(memory_space=pltpu.VMEM)
    return pl.pallas_call(
        lambda *refs: kernel(factor, *refs),
        name="reduced_step",
        out_shape=(jax.ShapeDtypeStruct((LM, NX * LM), f32), jax.ShapeDtypeStruct((8, 128), f32)),
        in_specs=[vmem] * 6 + [pl.BlockSpec(memory_space=pltpu.SMEM)],
        out_specs=(vmem, vmem),
        scratch_shapes=scratch,
        compiler_params=pltpu.CompilerParams(
            collective_id=0, has_side_effects=True, vmem_limit_bytes=40 * 1024 * 1024
        ),
    )(*operands)


def body(reduced_coords, mode_basis, rest_shape, stiffness, send_slots, pair_peer, pair_slot, pair_count):
    local_modes, _, vertex_count = mode_basis.shape
    factor = local_modes * NX / (3.0 * vertex_count * NZ * NS)
    basis = jnp.transpose(mode_basis, (1, 0, 2)).reshape(LC, NV)
    hi = lax.reduce_precision(reduced_coords, 8, 7)
    mid = lax.reduce_precision(reduced_coords - hi, 8, 7)
    lo = reduced_coords - hi - mid
    parts = jnp.stack([hi, mid, lo])
    eye = jnp.concatenate([jnp.eye(3, dtype=f32), jnp.zeros((5, 3), f32)])
    coeff = (parts[:, None, None, :] * eye[None, :, :, None]).reshape(24, LC).astype(bf16)
    slots = send_slots.reshape(NZ, NS * NSLOT)
    ends = (pair_peer * NSLOT + pair_slot).reshape(2, NPAIR)
    hessian, gradient = step(
        factor, basis, coeff, rest_shape, stiffness.reshape(1, NV), slots, ends, pair_count
    )
    return hessian, gradient[0, :LM]


def solution(mesh):
    finer = Mesh(mesh.devices.reshape(NZ, 4, 2, NX), ("z", "y", "c", "x"))
    placed = (
        P("x"),
        P("x", None, VERTS),
        P(None, VERTS),
        P(VERTS),
        P(VERTS, None, None),
        P(VERTS, None, None),
        P(VERTS, None, None),
        P(VERTS),
    )
    return jax.shard_map(
        body, mesh=finer, in_specs=placed, out_specs=(P("x", None), P("x")), check_vma=False
    )
```

```python
import jax
import jax.numpy as jnp
from jax import lax
from jax.experimental import pallas as pl
from jax.experimental.pallas import tpu as pltpu
from jax.sharding import Mesh
from jax.sharding import PartitionSpec as P

VERTS = ("z", "y", "c")
MESH = pl.DeviceIdType.MESH
NZ, NS, NX = 16, 8, 4
NP = NX * NS
LM, LC = 64, 192
NV, NPAIR, NSLOT = 1024, 1024, 16
Q = 256
ROWS = 24
GROUP = 4
SPANS = ((0, 1), (1, 2), (3, 4), (7, 9))
EARLY = 9
f32, bf16 = jnp.float32, jnp.bfloat16

barrier_reach = 1.5
gap_offset = 0.1


def split3(v):
    hi = v.astype(bf16).astype(f32)
    mid = (v - hi).astype(bf16).astype(f32)
    return hi, mid, v - hi - mid


def dot_nt(a, b):
    return lax.dot_general(a, b, (((1,), (1,)), ((), ())), preferred_element_type=f32)


def dot_nn(a, b):
    return lax.dot_general(a, b, (((1,), (0,)), ((), ())), preferred_element_type=f32)


def offset_of(n):
    m = (n + 1) // 2
    odd = m % 2
    hops = odd * ((m + 1) // 2) + (1 - odd) * (8 - m // 2)
    return ((n % 2) * hops + (1 - n % 2) * (NZ - hops)) * (1 - n // (NZ - 1))


def barrier_slopes(distance):
    excess = distance - barrier_reach
    ratio_log = jnp.log(distance / barrier_reach)
    slope_term = -(2.0 * excess * ratio_log + excess * excess / distance)
    curvature = -(2.0 * ratio_log + 4.0 * excess / distance - excess * excess / (distance * distance))
    inside = distance < barrier_reach
    return jnp.where(inside, slope_term, 0.0), jnp.where(inside, curvature, 0.0)


def accumulate(parts, s, scale, bend, hess, grad, exact):
    lever = jnp.zeros((NX * LM, Q), f32)
    total = None
    slopes = None
    for k in range(3):
        x = parts[k].astype(f32)
        xb = x.astype(bf16)
        sk = s[k : k + 1, :]
        lever = lever + x * sk
        part = dot_nt((x * scale).astype(bf16), xb)
        total = part if total is None else total + part
        hi, mid, lo = split3(scale * sk)
        force = jnp.concatenate([hi, mid, lo, jnp.zeros((13, Q), f32)], axis=0).astype(bf16)
        gpart = dot_nt(force, xb)
        if not exact:
            gpart = gpart + dot_nt(force, (x - xb.astype(f32)).astype(bf16))
        slopes = gpart if slopes is None else slopes + gpart
    total = total + dot_nt((lever * bend).astype(bf16), lever.astype(bf16))
    slopes = jnp.sum(slopes, axis=0, keepdims=True)
    if exact:
        hess[...] = total
        grad[...] = slopes
    else:
        hess[...] = hess[...] + total
        grad[...] = grad[...] + slopes


def kernel(
    factor,
    basis_hbm, coord_hbm, rest_hbm, stiff_hbm, slots_hbm, peer_hbm, seat_hbm, count_hbm,
    out_h, out_g,
    wide, coord, rest_v, stiff, slots, peer, seat, count,
    obuf, stage, rows_in, restg, restp, resta, restz,
    part_s, xb, xp, ends, acc, early_s, early_r, late_s, late_r, usend, xu,
    hess, grad, hsend, hplane, zsend, hz, csend, hc,
    in_sem, p1_s, p1_r, ri_s, ri_r, rz_s, rz_r, zm_s, zm_r,
    x_s, x_r, a_s, a_r, b_s, b_r, c_s, c_r,
):
    z, y, c, x = (lax.axis_index(n) for n in ("z", "y", "c", "x"))
    s = y * 2 + c
    p = x * NS + s

    def plane_peer(k):
        q = lax.rem(p + k, NP)
        sq = lax.rem(q, NS)
        return q, {"x": q // NS, "y": sq // 2, "c": lax.rem(sq, 2)}

    def near_peer(k):
        q = lax.rem(s + k, NS)
        return q, {"y": q // 2, "c": lax.rem(q, 2)}

    def remote(src, dst, ssem, rsem, where):
        return pltpu.make_async_remote_copy(src, dst, ssem, rsem, device_id=where, device_id_type=MESH)

    def arrived(ref, sem):
        remote(ref, ref, c_s, sem, {"z": z}).wait_recv()

    def left(ref, sem):
        remote(ref, ref, sem, c_r, {"z": z}).wait_send()

    bar = pltpu.get_barrier_semaphore()

    @pl.loop(1, NZ)
    def _(k):
        pl.semaphore_signal(bar, inc=1, device_id={"z": lax.rem(z + k, NZ)}, device_id_type=MESH)

    @pl.loop(1, NP)
    def _(k):
        pl.semaphore_signal(bar, inc=1, device_id=plane_peer(k)[1], device_id_type=MESH)

    loads = [
        pltpu.make_async_copy(src, dst, in_sem.at[i])
        for i, (src, dst) in enumerate(
            (
                (slots_hbm, slots), (basis_hbm, wide.at[pl.ds(0, LC)]), (rest_hbm, rest_v), (coord_hbm, coord),
                (stiff_hbm, stiff), (peer_hbm, peer), (seat_hbm, seat), (count_hbm, count),
            )
        )
    ]
    for load in loads:
        load.start()
    wide[LC:Q, :] = jnp.zeros((Q - LC, NV), bf16)
    for load in loads:
        load.wait()

    rest = rest_v[...]
    mine = jnp.where(x == 0, rest[0:1], jnp.where(x == 1, rest[1:2], jnp.where(x == 2, rest[2:3], 0.0)))
    hi, mid, lo = split3(mine)
    rest_rows = jnp.concatenate([hi, mid, lo, jnp.zeros((13, NV), f32)], axis=0).astype(bf16)
    lane = lax.broadcasted_iota(jnp.int32, (128, 128), 1)
    seat_of = lax.broadcasted_iota(jnp.int32, (128, 128), 0) // NSLOT
    listed = jnp.concatenate([slots[...].astype(f32)] * NS, axis=0)
    lanef = lane.astype(f32)

    @pl.loop(0, NZ // GROUP)
    def _(g):
        hots = []
        for i in range(GROUP):
            zq = lax.rem(z + offset_of(g * GROUP + i), NZ)
            col = jnp.sum(jnp.where(lane == seat_of + zq * NS, listed, 0.0), axis=1, keepdims=True)
            blocks = [jnp.where(col == lanef + 128.0 * b, 1.0, 0.0).astype(bf16) for b in range(NV // 128)]
            hots.append(jnp.concatenate(blocks, axis=1))
        hot = jnp.concatenate(hots, axis=0)
        picked = dot_nt(hot, wide[...])
        tail = picked[:, 128:256]
        turned = pltpu.roll(tail, 64, 1)
        tail = tail.reshape(GROUP * NS, 2, 8, 128)[:, 0] + turned.reshape(GROUP * NS, 2, 8, 128)[:, 1]
        chunk = jnp.concatenate([picked[:, 0:128].reshape(GROUP * NS, 16, 128), tail], axis=1)
        chunk = chunk.astype(bf16).reshape(GROUP, NS, ROWS, 128)
        rests = jnp.sum(dot_nt(rest_rows, hot), axis=0, keepdims=True)
        for i in range(GROUP):
            n = g * GROUP + i
            obuf[:, pl.ds(n, 1)] = chunk[i][:, None]
            restg[pl.ds(n, 1), :] = rests[:, 128 * i : 128 * (i + 1)]

    line = jnp.concatenate([coord[...]] * 3 + [jnp.zeros((1, Q - LC), f32)], axis=1)
    own_row = lax.broadcasted_iota(jnp.int32, (8, Q), 0) == lax.broadcasted_iota(jnp.int32, (8, Q), 1) // LM
    hi, mid, lo = split3(jnp.where(own_row, line, 0.0))
    coeff = jnp.concatenate([hi, mid, lo, jnp.zeros((8, Q), f32)], axis=0).astype(bf16)

    moved = dot_nn(coeff, wide[...])
    part_s[...] = moved[0:8] + moved[8:16] + moved[16:24]

    pl.semaphore_wait(bar, NZ - 1 + NP - 1)

    for g, (start, size) in enumerate(SPANS):

        @pl.loop(1, NS)
        def _(k):
            q, where = near_peer(k)
            span = pl.ds(start, size)
            remote(obuf.at[q, span], stage.at[span, s], p1_s.at[g], p1_r.at[g], where).start()

        if g == 0:

            @pl.loop(1, NS)
            def _(k):
                remote(restg, restp.at[s], ri_s, ri_r, near_peer(k)[1]).start()

    @pl.loop(1, NX)
    def _(k):
        q = lax.rem(x + k, NX)
        cols = pl.ds(pl.multiple_of(q * Q, Q), Q)
        remote(wide.at[pl.ds(0, LC), cols], xb.at[x], x_s.at[0], x_r.at[0], {"x": q}).start()
        remote(part_s.at[:, cols], xp.at[x], x_s.at[1], x_r.at[1], {"x": q}).start()

    own = pl.ds(pl.multiple_of(x * Q, Q), Q)
    stage[:, pl.ds(s, 1)] = obuf[s][:, None]
    restp[s] = restg[...]
    xb[x] = wide[0:LC, own]
    xp[x] = part_s[:, own]

    def toward(n):
        return {"z": lax.rem(z + offset_of(n), NZ)}

    for g, (start, size) in enumerate(SPANS):
        arrived(obuf.at[pl.ds(0, NS - 1), pl.ds(0, size)], p1_r.at[g])
        for n in range(start, min(start + size, NZ - 1)):
            remote(stage.at[n], rows_in.at[n], zm_s, zm_r.at[n], toward(n)).start()
        if g == 0:
            arrived(restp.at[pl.ds(0, NS - 1)], ri_r)
            place_of = lax.broadcasted_iota(jnp.int32, (NZ, 128), 1) // NSLOT
            gathered = jnp.zeros((NZ, 128), f32)
            for q in range(NS):
                shift = lax.rem((q - s + NS) * NSLOT, 128)
                gathered = jnp.where(place_of == q, pltpu.roll(restp[q], shift, 1), gathered)
            resta[...] = gathered.reshape(NZ, 1, 128)
            for n in range(NZ - 1):
                remote(resta.at[n], restz.at[n], rz_s, rz_r, toward(n)).start()
            restz[NZ - 1] = resta[NZ - 1]
    rows_in[NZ - 1] = stage[NZ - 1]

    for i, buf in enumerate((xb, xp)):
        arrived(buf.at[pl.ds(0, NX - 1)], x_r.at[i])
    disp = xp[0] + xp[1] + xp[2] + xp[3]
    square = 1.0 + disp[0:1] * disp[0:1] + disp[1:2] * disp[1:2] + disp[2:3] * disp[2:3]
    rate = stiff[:, own] / jnp.sqrt(square)
    columns = [xb[:, LM * k : LM * (k + 1), :].reshape(NX * LM, Q) for k in range(3)]
    accumulate(columns, disp, rate, -rate / square, hess, grad, True)

    acc[...] = jnp.zeros_like(acc)
    pick = lax.broadcasted_iota(jnp.int32, (8, 128), 0) == x
    code = lax.broadcasted_iota(jnp.int32, (128, NPAIR), 0)
    ends[...] = peer[...] * NSLOT + seat[...]
    arrived(resta.at[pl.ds(0, NZ - 1)], rz_r)

    def consume(n, awaited=True):
        base = lax.rem(z + NZ - offset_of(n), NZ) * 128
        first = jnp.where(ends[0:1, :] - base == code, 1.0, 0.0)
        second = jnp.where(ends[1:2, :] - base == code, 1.0, 0.0)
        choose = (first - second).astype(bf16)
        if awaited:
            arrived(stage.at[n], zm_r.at[n])
        got = rows_in[n].astype(f32)
        head = got[:, 0:16].reshape(128, 128)
        tail = got[:, 16:24]
        turned = pltpu.roll(tail.reshape(64, 128), 64, 1).reshape(NS, 1, 8, 128)
        tail = jnp.concatenate([tail.reshape(NS, 1, 8, 128), turned], axis=1).reshape(128, 128)
        cols = jnp.concatenate([jnp.transpose(head), jnp.transpose(tail)[0:LM]], axis=0).astype(bf16)
        pos = dot_nn(coeff[:, 0:LC], cols)
        pos = pos[0:8] + pos[8:16] + pos[16:24] + jnp.where(pick, restz[n], 0.0)
        hi, mid, lo = split3(pos)
        pos = jnp.concatenate([hi, mid, lo, jnp.zeros((8, 128), f32)], axis=0).astype(bf16)
        acc[...] = acc[...] + dot_nn(jnp.concatenate([cols, pos], axis=0), choose)

    def hand_out(src, dst, i):
        @pl.loop(1, NX)
        def _(k):
            q = lax.rem(x + k, NX)
            cols = pl.ds(pl.multiple_of(q * Q, Q), Q)
            remote(src.at[:, cols], dst.at[x], x_s.at[i], x_r.at[i], {"x": q}).start()

        dst[x] = src[:, own]

    consume(NZ - 1, False)

    @pl.loop(0, EARLY)
    def _(n):
        consume(n)

    diff = acc[0:LC, :]
    high = diff.astype(bf16)
    early_s[0:LC, :] = high
    early_s[LC : 2 * LC, :] = (diff - high.astype(f32)).astype(bf16)
    hand_out(early_s, early_r, 4)
    acc[0:LC, :] = jnp.zeros((LC, NPAIR), f32)

    @pl.loop(EARLY, NZ - 1)
    def _(n):
        consume(n)

    usend[...] = acc[LC : LC + 8, :] + acc[LC + 8 : LC + 16, :] + acc[LC + 16 : LC + 24, :]
    hand_out(usend, xu, 3)
    late_s[...] = acc[0:LC, :].astype(bf16)
    hand_out(late_s, late_r, 2)
    arrived(xu.at[pl.ds(0, NX - 1)], x_r.at[3])
    gap = xu[0] + xu[1] + xu[2] + xu[3]
    distance = gap[0:1] * gap[0:1] + gap[1:2] * gap[1:2] + gap[2:3] * gap[2:3] + gap_offset
    slope, bend = barrier_slopes(distance)
    live = lax.broadcasted_iota(jnp.int32, (1, Q), 1) + x * Q < count[...]
    slope = jnp.where(live, slope, 0.0)
    bend = jnp.where(live, bend, 0.0)
    arrived(early_r.at[pl.ds(0, NX - 1)], x_r.at[4])
    known = early_r[:, 0:LC].astype(f32) + early_r[:, LC : 2 * LC].astype(f32)
    arrived(late_r.at[pl.ds(0, NX - 1)], x_r.at[2])
    known = known + late_r[...].astype(f32)
    columns = [known[:, LM * k : LM * (k + 1)].reshape(NX * LM, Q) for k in range(3)]
    accumulate(columns, gap, 2.0 * slope, 4.0 * bend, hess, grad, False)

    def packed_grad(row):
        hi = row.astype(bf16).astype(f32)
        lo = row - hi
        return jnp.concatenate(
            [hi[:, 0:128], hi[:, 128:256], lo[:, 0:128], lo[:, 128:256], jnp.zeros((4, 128), f32)], axis=0
        )

    h = hess[...]
    tail = jnp.broadcast_to(packed_grad(grad[...])[None], (NP, 8, 128))
    hsend[...] = jnp.concatenate(
        [h[:, 0:128].reshape(NP, 8, 128), h[:, 128:256].reshape(NP, 8, 128), tail], axis=1
    ).astype(bf16)

    @pl.loop(1, NP)
    def _(k):
        q, where = plane_peer(k)
        remote(hsend.at[q], hplane.at[p], a_s, a_r, where).start()

    hplane[p] = hsend[p]
    arrived(hsend.at[pl.ds(0, NP - 1)], a_r)
    total = jnp.sum(hplane[...].astype(f32), axis=0)
    g0, g1 = total[16:17] + total[18:19], total[17:18] + total[19:20]
    zsend[...] = jnp.concatenate([total[0:16], packed_grad(jnp.concatenate([g0, g1], axis=1))], axis=0).astype(bf16)

    @pl.loop(1, NZ)
    def _(k):
        remote(zsend, hz.at[z], b_s, b_r, {"z": lax.rem(z + k, NZ)}).start()

    hz[z] = zsend[...]
    arrived(hz.at[pl.ds(0, NZ - 1)], b_r)
    total = jnp.sum(hz[...].astype(f32), axis=0) * factor
    csend[...] = total[0:16]

    @pl.loop(1, NS)
    def _(k):
        remote(csend, hc.at[s], c_s, c_r, near_peer(k)[1]).start()

    hc[s] = csend[...]
    g0, g1 = total[16:17] + total[18:19], total[17:18] + total[19:20]
    half = jnp.broadcast_to(jnp.where(x >= 2, g1, g0), (8, 128))
    half = jnp.where(lax.rem(x, 2) == 1, pltpu.roll(half, 64, 1), half)
    out_g[...] = half[0:1, 0:LM]

    for g, (_start, size) in enumerate(SPANS):
        left(obuf.at[pl.ds(0, NS - 1), pl.ds(0, size)], p1_s.at[g])
    for src, sem in (
        (restp.at[pl.ds(0, NS - 1)], ri_s),
        (resta.at[pl.ds(0, NZ - 1)], rz_s),
        (stage.at[pl.ds(0, NZ - 1)], zm_s),
        (xb.at[pl.ds(0, NX - 1)], x_s.at[0]),
        (xp.at[pl.ds(0, NX - 1)], x_s.at[1]),
        (late_r.at[pl.ds(0, NX - 1)], x_s.at[2]),
        (xu.at[pl.ds(0, NX - 1)], x_s.at[3]),
        (early_r.at[pl.ds(0, NX - 1)], x_s.at[4]),
        (hsend.at[pl.ds(0, NP - 1)], a_s),
        (hz.at[pl.ds(0, NZ - 1)], b_s),
        (hc.at[pl.ds(0, NS - 1)], c_s),
    ):
        left(src, sem)

    arrived(hc.at[pl.ds(0, NS - 1)], c_r)
    out_h[:, 0:128] = hc[:, 0:8, :].reshape(LM, 128)
    out_h[:, 128:256] = hc[:, 8:16, :].reshape(LM, 128)


def step(factor, *operands):
    dma = pltpu.SemaphoreType.DMA
    i32 = jnp.int32
    scratch = [
        pltpu.VMEM((Q, NV), bf16),
        pltpu.VMEM((1, LM), f32),
        pltpu.VMEM((3, NV), f32),
        pltpu.VMEM((1, NV), f32),
        pltpu.VMEM((NSLOT, NZ * NS), i32),
        pltpu.VMEM((2, NPAIR), i32),
        pltpu.VMEM((2, NPAIR), i32),
        pltpu.VMEM((1, 1), i32),
        pltpu.VMEM((NS, NZ, ROWS, 128), bf16),
        pltpu.VMEM((NZ, NS, ROWS, 128), bf16),
        pltpu.VMEM((NZ, NS, ROWS, 128), bf16),
        pltpu.VMEM((NZ, 128), f32),
        pltpu.VMEM((NS, NZ, 128), f32),
        pltpu.VMEM((NZ, 1, 128), f32),
        pltpu.VMEM((NZ, 1, 128), f32),
        pltpu.VMEM((8, NV), f32),
        pltpu.VMEM((NX, LC, Q), bf16),
        pltpu.VMEM((NX, 8, Q), f32),
        pltpu.VMEM((2, NPAIR), i32),
        pltpu.VMEM((LC + 32, NPAIR), f32),
        pltpu.VMEM((2 * LC, NPAIR), bf16),
        pltpu.VMEM((NX, 2 * LC, Q), bf16),
        pltpu.VMEM((LC, NPAIR), bf16),
        pltpu.VMEM((NX, LC, Q), bf16),
        pltpu.VMEM((8, NPAIR), f32),
        pltpu.VMEM((NX, 8, Q), f32),
        pltpu.VMEM((NX * LM, NX * LM), f32),
        pltpu.VMEM((1, NX * LM), f32),
        pltpu.VMEM((NP, ROWS, 128), bf16),
        pltpu.VMEM((NP, ROWS, 128), bf16),
        pltpu.VMEM((ROWS, 128), bf16),
        pltpu.VMEM((NZ, ROWS, 128), bf16),
        pltpu.VMEM((16, 128), f32),
        pltpu.VMEM((NS, 16, 128), f32),
        dma((8,)), dma((len(SPANS),)), dma((len(SPANS),)), dma, dma, dma, dma, dma, dma((NZ,)),
        dma((5,)), dma((5,)), dma, dma, dma, dma, dma, dma,
    ]
    vmem = pl.BlockSpec(memory_space=pltpu.VMEM)
    return pl.pallas_call(
        lambda *refs: kernel(factor, *refs),
        name="reduced_step",
        out_shape=(jax.ShapeDtypeStruct((LM, NX * LM), f32), jax.ShapeDtypeStruct((1, LM), f32)),
        in_specs=[pl.BlockSpec(memory_space=pltpu.HBM)] * 8,
        out_specs=(vmem, vmem),
        scratch_shapes=scratch,
        compiler_params=pltpu.CompilerParams(
            collective_id=0, has_side_effects=True, vmem_limit_bytes=56 * 1024 * 1024
        ),
    )(*operands)


def body(reduced_coords, mode_basis, rest_shape, stiffness, send_slots, pair_peer, pair_slot, pair_count):
    local_modes, _, vertex_count = mode_basis.shape
    factor = local_modes * NX / (3.0 * vertex_count * NZ * NS)
    hessian, gradient = step(
        factor,
        jnp.transpose(mode_basis, (1, 0, 2)).reshape(LC, NV),
        reduced_coords.reshape(1, LM),
        rest_shape,
        stiffness.reshape(1, NV),
        jnp.transpose(send_slots[0]),
        pair_peer[0],
        pair_slot[0],
        pair_count.reshape(1, 1),
    )
    return hessian, gradient.reshape(LM)


def solution(mesh):
    finer = Mesh(mesh.devices.reshape(NZ, 4, 2, NX), ("z", "y", "c", "x"))
    placed = (
        P("x"),
        P("x", None, VERTS),
        P(None, VERTS),
        P(VERTS),
        P(VERTS, None, None),
        P(VERTS, None, None),
        P(VERTS, None, None),
        P(VERTS),
    )
    return jax.shard_map(
        body, mesh=finer, in_specs=placed, out_specs=(P("x", None), P("x")), check_vma=False
    )
```

```python
import jax
import jax.numpy as jnp
from jax import lax
from jax.experimental import pallas as pl
from jax.experimental.pallas import tpu as pltpu
from jax.sharding import Mesh
from jax.sharding import PartitionSpec as P

VERTS = ("z", "y", "c")
MESH = pl.DeviceIdType.MESH
NZ, NS, NX = 16, 8, 4
NP = NX * NS
LM, LC = 64, 192
NV, NPAIR, NSLOT = 1024, 1024, 16
Q = 256
ROWS = 24
GROUP = 4
SPANS = ((1, 2), (3, 4), (7, 9))
EARLY = 9
f32, bf16 = jnp.float32, jnp.bfloat16

barrier_reach = 1.5
gap_offset = 0.1


def split3(v):
    hi = v.astype(bf16).astype(f32)
    mid = (v - hi).astype(bf16).astype(f32)
    return hi, mid, v - hi - mid


def dot_nt(a, b):
    return lax.dot_general(a, b, (((1,), (1,)), ((), ())), preferred_element_type=f32)


def dot_nn(a, b):
    return lax.dot_general(a, b, (((1,), (0,)), ((), ())), preferred_element_type=f32)


def offset_of(n):
    m = (n + 1) // 2
    odd = m % 2
    hops = odd * ((m + 1) // 2) + (1 - odd) * (8 - m // 2)
    return ((n % 2) * hops + (1 - n % 2) * (NZ - hops)) * (1 - n // (NZ - 1))


def barrier_slopes(distance):
    excess = distance - barrier_reach
    ratio_log = jnp.log(distance / barrier_reach)
    slope_term = -(2.0 * excess * ratio_log + excess * excess / distance)
    curvature = -(2.0 * ratio_log + 4.0 * excess / distance - excess * excess / (distance * distance))
    inside = distance < barrier_reach
    return jnp.where(inside, slope_term, 0.0), jnp.where(inside, curvature, 0.0)


def accumulate(parts, s, scale, bend, hess, grad, exact):
    lever = jnp.zeros((NX * LM, Q), f32)
    total = None
    slopes = None
    for k in range(3):
        x = parts[k].astype(f32)
        xb = x.astype(bf16)
        sk = s[k : k + 1, :]
        lever = lever + x * sk
        part = dot_nt((x * scale).astype(bf16), xb)
        total = part if total is None else total + part
        hi, mid, lo = split3(scale * sk)
        force = jnp.concatenate([hi, mid, lo, jnp.zeros((13, Q), f32)], axis=0).astype(bf16)
        gpart = dot_nt(force, xb)
        if not exact:
            gpart = gpart + dot_nt(force, (x - xb.astype(f32)).astype(bf16))
        slopes = gpart if slopes is None else slopes + gpart
    total = total + dot_nt((lever * bend).astype(bf16), lever.astype(bf16))
    slopes = jnp.sum(slopes, axis=0, keepdims=True)
    if exact:
        hess[...] = total
        grad[...] = slopes
    else:
        hess[...] = hess[...] + total
        grad[...] = grad[...] + slopes


def kernel(
    factor,
    basis_hbm, coord_hbm, rest_hbm, stiff_hbm, slots_hbm, peer_hbm, seat_hbm, count_hbm,
    out_h, out_g,
    wide, coord, rest_v, stiff, slots, peer, seat, count,
    obuf, stage, rows_in, restg, restp, resta, restz,
    part_s, xb, xp, ends, acc, early_s, early_r, late_s, late_r, usend, xu,
    hess, grad, hsend, hplane, zsend, hz, csend, hc,
    in_sem, p1_s, p1_r, ri_s, ri_r, rz_s, rz_r, zm_s, zm_r,
    x_s, x_r, a_s, a_r, b_s, b_r, c_s, c_r,
):
    z, y, c, x = (lax.axis_index(n) for n in ("z", "y", "c", "x"))
    s = y * 2 + c
    p = x * NS + s

    def plane_peer(k):
        q = lax.rem(p + k, NP)
        sq = lax.rem(q, NS)
        return q, {"x": q // NS, "y": sq // 2, "c": lax.rem(sq, 2)}

    def near_peer(k):
        q = lax.rem(s + k, NS)
        return q, {"y": q // 2, "c": lax.rem(q, 2)}

    def far_peer(k):
        q, where = near_peer(k)
        return q, {"z": lax.rem(z + offset_of(0), NZ), **where}

    def remote(src, dst, ssem, rsem, where):
        return pltpu.make_async_remote_copy(src, dst, ssem, rsem, device_id=where, device_id_type=MESH)

    def arrived(ref, sem):
        remote(ref, ref, c_s, sem, {"z": z}).wait_recv()

    def left(ref, sem):
        remote(ref, ref, sem, c_r, {"z": z}).wait_send()

    bar = pltpu.get_barrier_semaphore()

    @pl.loop(1, NZ)
    def _(k):
        pl.semaphore_signal(bar, inc=1, device_id={"z": lax.rem(z + k, NZ)}, device_id_type=MESH)

    @pl.loop(1, NS)
    def _(k):
        pl.semaphore_signal(bar, inc=1, device_id=far_peer(k)[1], device_id_type=MESH)

    @pl.loop(1, NP)
    def _(k):
        pl.semaphore_signal(bar, inc=1, device_id=plane_peer(k)[1], device_id_type=MESH)

    loads = [
        pltpu.make_async_copy(src, dst, in_sem.at[i])
        for i, (src, dst) in enumerate(
            (
                (slots_hbm, slots), (basis_hbm, wide.at[pl.ds(0, LC)]), (rest_hbm, rest_v), (coord_hbm, coord),
                (stiff_hbm, stiff), (peer_hbm, peer), (seat_hbm, seat), (count_hbm, count),
            )
        )
    ]
    for load in loads:
        load.start()
    wide[LC:Q, :] = jnp.zeros((Q - LC, NV), bf16)
    for load in loads:
        load.wait()

    rest = rest_v[...]
    mine = jnp.where(x == 0, rest[0:1], jnp.where(x == 1, rest[1:2], jnp.where(x == 2, rest[2:3], 0.0)))
    hi, mid, lo = split3(mine)
    rest_rows = jnp.concatenate([hi, mid, lo, jnp.zeros((13, NV), f32)], axis=0).astype(bf16)
    lane = lax.broadcasted_iota(jnp.int32, (128, 128), 1)
    seat_of = lax.broadcasted_iota(jnp.int32, (128, 128), 0) // NSLOT
    listed = jnp.concatenate([slots[...].astype(f32)] * NS, axis=0)
    lanef = lane.astype(f32)

    @pl.loop(0, NZ // GROUP)
    def _(g):
        hots = []
        for i in range(GROUP):
            zq = lax.rem(z + offset_of(g * GROUP + i), NZ)
            col = jnp.sum(jnp.where(lane == seat_of + zq * NS, listed, 0.0), axis=1, keepdims=True)
            blocks = [jnp.where(col == lanef + 128.0 * b, 1.0, 0.0).astype(bf16) for b in range(NV // 128)]
            hots.append(jnp.concatenate(blocks, axis=1))
        hot = jnp.concatenate(hots, axis=0)
        picked = dot_nt(hot, wide[...])
        tail = picked[:, 128:256]
        turned = pltpu.roll(tail, 64, 1)
        tail = tail.reshape(GROUP * NS, 2, 8, 128)[:, 0] + turned.reshape(GROUP * NS, 2, 8, 128)[:, 1]
        chunk = jnp.concatenate([picked[:, 0:128].reshape(GROUP * NS, 16, 128), tail], axis=1)
        chunk = chunk.astype(bf16).reshape(GROUP, NS, ROWS, 128)
        rests = jnp.sum(dot_nt(rest_rows, hot), axis=0, keepdims=True)
        for i in range(GROUP):
            n = g * GROUP + i
            obuf[:, pl.ds(n, 1)] = chunk[i][:, None]
            restg[pl.ds(n, 1), :] = rests[:, 128 * i : 128 * (i + 1)]

    line = jnp.concatenate([coord[...]] * 3 + [jnp.zeros((1, Q - LC), f32)], axis=1)
    own_row = lax.broadcasted_iota(jnp.int32, (8, Q), 0) == lax.broadcasted_iota(jnp.int32, (8, Q), 1) // LM
    hi, mid, lo = split3(jnp.where(own_row, line, 0.0))
    coeff = jnp.concatenate([hi, mid, lo, jnp.zeros((8, Q), f32)], axis=0).astype(bf16)

    moved = dot_nn(coeff, wide[...])
    part_s[...] = moved[0:8] + moved[8:16] + moved[16:24]

    pl.semaphore_wait(bar, NZ - 1 + NP - 1 + NS - 1)

    @pl.loop(0, NS)
    def _(k):
        q, where = far_peer(k)
        remote(obuf.at[q, 0], rows_in.at[0, s], zm_s, zm_r.at[0], where).start()

    for g, (start, size) in enumerate(SPANS):

        @pl.loop(1, NS)
        def _(k):
            q, where = near_peer(k)
            span = pl.ds(start, size)
            remote(obuf.at[q, span], stage.at[span, s], p1_s.at[g], p1_r.at[g], where).start()

        if g == 0:

            @pl.loop(1, NS)
            def _(k):
                remote(restg, restp.at[s], ri_s, ri_r, near_peer(k)[1]).start()

    @pl.loop(1, NX)
    def _(k):
        q = lax.rem(x + k, NX)
        cols = pl.ds(pl.multiple_of(q * Q, Q), Q)
        remote(wide.at[pl.ds(0, LC), cols], xb.at[x], x_s.at[0], x_r.at[0], {"x": q}).start()
        remote(part_s.at[:, cols], xp.at[x], x_s.at[1], x_r.at[1], {"x": q}).start()

    own = pl.ds(pl.multiple_of(x * Q, Q), Q)
    stage[:, pl.ds(s, 1)] = obuf[s][:, None]
    restp[s] = restg[...]
    xb[x] = wide[0:LC, own]
    xp[x] = part_s[:, own]

    def toward(n):
        return {"z": lax.rem(z + offset_of(n), NZ)}

    for g, (start, size) in enumerate(SPANS):
        arrived(obuf.at[pl.ds(0, NS - 1), pl.ds(0, size)], p1_r.at[g])
        for n in range(start, min(start + size, NZ - 1)):
            remote(stage.at[n], rows_in.at[n], zm_s, zm_r.at[n], toward(n)).start()
        if g == 0:
            arrived(restp.at[pl.ds(0, NS - 1)], ri_r)
            place_of = lax.broadcasted_iota(jnp.int32, (NZ, 128), 1) // NSLOT
            gathered = jnp.zeros((NZ, 128), f32)
            for q in range(NS):
                shift = lax.rem((q - s + NS) * NSLOT, 128)
                gathered = jnp.where(place_of == q, pltpu.roll(restp[q], shift, 1), gathered)
            resta[...] = gathered.reshape(NZ, 1, 128)
            for n in range(NZ - 1):
                remote(resta.at[n], restz.at[n], rz_s, rz_r, toward(n)).start()
            restz[NZ - 1] = resta[NZ - 1]
    rows_in[NZ - 1] = stage[NZ - 1]

    for i, buf in enumerate((xb, xp)):
        arrived(buf.at[pl.ds(0, NX - 1)], x_r.at[i])
    disp = xp[0] + xp[1] + xp[2] + xp[3]
    square = 1.0 + disp[0:1] * disp[0:1] + disp[1:2] * disp[1:2] + disp[2:3] * disp[2:3]
    rate = stiff[:, own] / jnp.sqrt(square)
    columns = [xb[:, LM * k : LM * (k + 1), :].reshape(NX * LM, Q) for k in range(3)]
    accumulate(columns, disp, rate, -rate / square, hess, grad, True)

    acc[...] = jnp.zeros_like(acc)
    pick = lax.broadcasted_iota(jnp.int32, (8, 128), 0) == x
    code = lax.broadcasted_iota(jnp.int32, (128, NPAIR), 0)
    ends[...] = peer[...] * NSLOT + seat[...]
    arrived(resta.at[pl.ds(0, NZ - 1)], rz_r)

    def consume(n, awaited=True):
        base = lax.rem(z + NZ - offset_of(n), NZ) * 128
        first = jnp.where(ends[0:1, :] - base == code, 1.0, 0.0)
        second = jnp.where(ends[1:2, :] - base == code, 1.0, 0.0)
        choose = (first - second).astype(bf16)
        if awaited:
            arrived(stage.at[n], zm_r.at[n])
        got = rows_in[n].astype(f32)
        head = got[:, 0:16].reshape(128, 128)
        tail = got[:, 16:24]
        turned = pltpu.roll(tail.reshape(64, 128), 64, 1).reshape(NS, 1, 8, 128)
        tail = jnp.concatenate([tail.reshape(NS, 1, 8, 128), turned], axis=1).reshape(128, 128)
        cols = jnp.concatenate([jnp.transpose(head), jnp.transpose(tail)[0:LM]], axis=0).astype(bf16)
        pos = dot_nn(coeff[:, 0:LC], cols)
        pos = pos[0:8] + pos[8:16] + pos[16:24] + jnp.where(pick, restz[n], 0.0)
        hi, mid, lo = split3(pos)
        pos = jnp.concatenate([hi, mid, lo, jnp.zeros((8, 128), f32)], axis=0).astype(bf16)
        acc[...] = acc[...] + dot_nn(jnp.concatenate([cols, pos], axis=0), choose)

    def hand_out(src, dst, i):
        @pl.loop(1, NX)
        def _(k):
            q = lax.rem(x + k, NX)
            cols = pl.ds(pl.multiple_of(q * Q, Q), Q)
            remote(src.at[:, cols], dst.at[x], x_s.at[i], x_r.at[i], {"x": q}).start()

        dst[x] = src[:, own]

    consume(NZ - 1, False)

    @pl.loop(0, EARLY)
    def _(n):
        consume(n)

    diff = acc[0:LC, :]
    high = diff.astype(bf16)
    early_s[0:LC, :] = high
    early_s[LC : 2 * LC, :] = (diff - high.astype(f32)).astype(bf16)
    hand_out(early_s, early_r, 4)
    acc[0:LC, :] = jnp.zeros((LC, NPAIR), f32)

    @pl.loop(EARLY, NZ - 1)
    def _(n):
        consume(n)

    usend[...] = acc[LC : LC + 8, :] + acc[LC + 8 : LC + 16, :] + acc[LC + 16 : LC + 24, :]
    hand_out(usend, xu, 3)
    late_s[...] = acc[0:LC, :].astype(bf16)
    hand_out(late_s, late_r, 2)
    arrived(xu.at[pl.ds(0, NX - 1)], x_r.at[3])
    gap = xu[0] + xu[1] + xu[2] + xu[3]
    distance = gap[0:1] * gap[0:1] + gap[1:2] * gap[1:2] + gap[2:3] * gap[2:3] + gap_offset
    slope, bend = barrier_slopes(distance)
    live = lax.broadcasted_iota(jnp.int32, (1, Q), 1) + x * Q < count[0]
    slope = jnp.where(live, slope, 0.0)
    bend = jnp.where(live, bend, 0.0)
    arrived(early_r.at[pl.ds(0, NX - 1)], x_r.at[4])
    known = early_r[:, 0:LC].astype(f32) + early_r[:, LC : 2 * LC].astype(f32)
    arrived(late_r.at[pl.ds(0, NX - 1)], x_r.at[2])
    known = known + late_r[...].astype(f32)
    columns = [known[:, LM * k : LM * (k + 1)].reshape(NX * LM, Q) for k in range(3)]
    accumulate(columns, gap, 2.0 * slope, 4.0 * bend, hess, grad, False)

    def packed_grad(row):
        hi = row.astype(bf16).astype(f32)
        lo = row - hi
        return jnp.concatenate(
            [hi[:, 0:128], hi[:, 128:256], lo[:, 0:128], lo[:, 128:256], jnp.zeros((4, 128), f32)], axis=0
        )

    h = hess[...]
    tail = jnp.broadcast_to(packed_grad(grad[...])[None], (NP, 8, 128))
    hsend[...] = jnp.concatenate(
        [h[:, 0:128].reshape(NP, 8, 128), h[:, 128:256].reshape(NP, 8, 128), tail], axis=1
    ).astype(bf16)

    @pl.loop(1, NP)
    def _(k):
        q, where = plane_peer(k)
        remote(hsend.at[q], hplane.at[p], a_s, a_r, where).start()

    hplane[p] = hsend[p]
    arrived(hsend.at[pl.ds(0, NP - 1)], a_r)
    total = jnp.sum(hplane[...].astype(f32), axis=0)
    g0, g1 = total[16:17] + total[18:19], total[17:18] + total[19:20]
    zsend[...] = jnp.concatenate([total[0:16], packed_grad(jnp.concatenate([g0, g1], axis=1))], axis=0).astype(bf16)

    @pl.loop(1, NZ)
    def _(k):
        remote(zsend, hz.at[z], b_s, b_r, {"z": lax.rem(z + k, NZ)}).start()

    hz[z] = zsend[...]
    arrived(hz.at[pl.ds(0, NZ - 1)], b_r)
    total = jnp.sum(hz[...].astype(f32), axis=0) * factor
    csend[...] = total[0:16]

    @pl.loop(1, NS)
    def _(k):
        remote(csend, hc.at[s], c_s, c_r, near_peer(k)[1]).start()

    hc[s] = csend[...]
    g0, g1 = total[16:17] + total[18:19], total[17:18] + total[19:20]
    half = jnp.broadcast_to(jnp.where(x >= 2, g1, g0), (8, 128))
    half = jnp.where(lax.rem(x, 2) == 1, pltpu.roll(half, 64, 1), half)
    out_g[...] = half[0:1, 0:LM]

    for g, (_start, size) in enumerate(SPANS):
        left(obuf.at[pl.ds(0, NS - 1), pl.ds(0, size)], p1_s.at[g])
    for src, sem in (
        (restp.at[pl.ds(0, NS - 1)], ri_s),
        (resta.at[pl.ds(0, NZ - 1)], rz_s),
        (stage.at[pl.ds(0, NZ - 1)], zm_s),
        (xb.at[pl.ds(0, NX - 1)], x_s.at[0]),
        (xp.at[pl.ds(0, NX - 1)], x_s.at[1]),
        (late_r.at[pl.ds(0, NX - 1)], x_s.at[2]),
        (xu.at[pl.ds(0, NX - 1)], x_s.at[3]),
        (early_r.at[pl.ds(0, NX - 1)], x_s.at[4]),
        (hsend.at[pl.ds(0, NP - 1)], a_s),
        (hz.at[pl.ds(0, NZ - 1)], b_s),
        (hc.at[pl.ds(0, NS - 1)], c_s),
    ):
        left(src, sem)

    arrived(hc.at[pl.ds(0, NS - 1)], c_r)
    out_h[:, 0:128] = hc[:, 0:8, :].reshape(LM, 128)
    out_h[:, 128:256] = hc[:, 8:16, :].reshape(LM, 128)


def step(factor, *operands):
    dma = pltpu.SemaphoreType.DMA
    i32 = jnp.int32
    scratch = [
        pltpu.VMEM((Q, NV), bf16),
        pltpu.VMEM((1, LM), f32),
        pltpu.VMEM((3, NV), f32),
        pltpu.VMEM((1, NV), f32),
        pltpu.VMEM((NSLOT, NZ * NS), i32),
        pltpu.VMEM((2, NPAIR), i32),
        pltpu.VMEM((2, NPAIR), i32),
        pltpu.SMEM((1,), i32),
        pltpu.VMEM((NS, NZ, ROWS, 128), bf16),
        pltpu.VMEM((NZ, NS, ROWS, 128), bf16),
        pltpu.VMEM((NZ, NS, ROWS, 128), bf16),
        pltpu.VMEM((NZ, 128), f32),
        pltpu.VMEM((NS, NZ, 128), f32),
        pltpu.VMEM((NZ, 1, 128), f32),
        pltpu.VMEM((NZ, 1, 128), f32),
        pltpu.VMEM((8, NV), f32),
        pltpu.VMEM((NX, LC, Q), bf16),
        pltpu.VMEM((NX, 8, Q), f32),
        pltpu.VMEM((2, NPAIR), i32),
        pltpu.VMEM((LC + 32, NPAIR), f32),
        pltpu.VMEM((2 * LC, NPAIR), bf16),
        pltpu.VMEM((NX, 2 * LC, Q), bf16),
        pltpu.VMEM((LC, NPAIR), bf16),
        pltpu.VMEM((NX, LC, Q), bf16),
        pltpu.VMEM((8, NPAIR), f32),
        pltpu.VMEM((NX, 8, Q), f32),
        pltpu.VMEM((NX * LM, NX * LM), f32),
        pltpu.VMEM((1, NX * LM), f32),
        pltpu.VMEM((NP, ROWS, 128), bf16),
        pltpu.VMEM((NP, ROWS, 128), bf16),
        pltpu.VMEM((ROWS, 128), bf16),
        pltpu.VMEM((NZ, ROWS, 128), bf16),
        pltpu.VMEM((16, 128), f32),
        pltpu.VMEM((NS, 16, 128), f32),
        dma((8,)), dma((len(SPANS),)), dma((len(SPANS),)), dma, dma, dma, dma, dma, dma((NZ,)),
        dma((5,)), dma((5,)), dma, dma, dma, dma, dma, dma,
    ]
    vmem = pl.BlockSpec(memory_space=pltpu.VMEM)
    return pl.pallas_call(
        lambda *refs: kernel(factor, *refs),
        name="reduced_step",
        out_shape=(jax.ShapeDtypeStruct((LM, NX * LM), f32), jax.ShapeDtypeStruct((1, LM), f32)),
        in_specs=[pl.BlockSpec(memory_space=pltpu.HBM)] * 8,
        out_specs=(vmem, vmem),
        scratch_shapes=scratch,
        compiler_params=pltpu.CompilerParams(
            collective_id=0, has_side_effects=True, vmem_limit_bytes=56 * 1024 * 1024
        ),
    )(*operands)


def body(reduced_coords, mode_basis, rest_shape, stiffness, send_slots, pair_peer, pair_slot, pair_count):
    local_modes, _, vertex_count = mode_basis.shape
    factor = local_modes * NX / (3.0 * vertex_count * NZ * NS)
    hessian, gradient = step(
        factor,
        jnp.transpose(mode_basis, (1, 0, 2)).reshape(LC, NV),
        reduced_coords.reshape(1, LM),
        rest_shape,
        stiffness.reshape(1, NV),
        jnp.transpose(send_slots[0]),
        pair_peer[0],
        pair_slot[0],
        pair_count,
    )
    return hessian, gradient.reshape(LM)


def solution(mesh):
    finer = Mesh(mesh.devices.reshape(NZ, 4, 2, NX), ("z", "y", "c", "x"))
    placed = (
        P("x"),
        P("x", None, VERTS),
        P(None, VERTS),
        P(VERTS),
        P(VERTS, None, None),
        P(VERTS, None, None),
        P(VERTS, None, None),
        P(VERTS),
    )
    return jax.shard_map(
        body, mesh=finer, in_specs=placed, out_specs=(P("x", None), P("x")), check_vma=False
    )
```
